32 devices in a mesh: seq: 16 (over z, y, x), head: 2 (over core).
Axes of the slice: x: 2, y: 2, z: 4, core: 2. Of those that a mesh axis runs over, the one named last changes fastest.
Arguments:
- queries: bfloat16 [4096, 4096], P('seq', 'head'), may hold values from -210 to 210
- keys: bfloat16 [4096, 1024], P('seq', 'head'), may hold values from -7 to 7
- values: bfloat16 [4096, 1024], P('seq', 'head'), may hold values from -6 to 6
- vertical: int32 [8, 16], P('head'), may hold values from 0 to 63, as said below
- slash: int32 [8, 2], P('head'), may hold values from 1 to 4, as said below
- out_weight: bfloat16 [4096, 4096], P('head'), may hold values from -1 to 1
Outputs:
- mixed: bfloat16 [4096, 4096], P(('seq', 'head'))
The draws below stay inside these ranges and needn't reach their ends.
Inputs may be any that keep to these rules, and one draw needn't show every extreme that they name: `vertical`: for each key-value head, 16 different key blocks in increasing order; block b lies in slab b // 4; no slab holds more than 2 of one head's blocks, and for every head some slab holds exactly 2. `slash`: for each key-value head, 2 different offsets in increasing order; some head has the offset 256 // 64.
All inputs are finite; a program needn't handle non-finite values.
Results may differ from the reference program's by a relative error of at most 0.01.
Values may be sent and summed in bfloat16 or wider, within the bound.
A program may use at most 128 MiB of HBM per device.

```python
from functools import partial
import jax
import jax.numpy as jnp
from jax import lax

HEADS = 32
KEY_VALUE_HEADS = 8
HEAD_DIM = 128
DMODEL = 4096
S_DEV = 256
BLK = 64
NS = 2
CAP = 2
NV = 16
SEQ = 4096
N_SEQ = 16


def paired(key):
    key_seed, query_seed = jax.random.split(jax.random.fold_in(key, 7), 2)
    keys_f = jnp.clip(jax.random.normal(key_seed, (SEQ, KEY_VALUE_HEADS * HEAD_DIM), jnp.float32), -6.0, 6.0)
    query_f = jnp.clip(1.5 * jax.random.normal(query_seed, (SEQ, HEADS * HEAD_DIM), jnp.float32), -9.0, 9.0)
    return (query_f, keys_f)


def draw_queries(key, part):
    return paired(key)[0].astype(jnp.bfloat16)


def draw_keys(key, part):
    return paired(key)[1].astype(jnp.bfloat16)


def draw_vertical(key, part):
    block_span = S_DEV // BLK
    owners = SEQ // S_DEV
    perm_seed, score_seed, force_seed = jax.random.split(jax.random.fold_in(key, 3), 3)
    within = jax.random.randint(perm_seed, (KEY_VALUE_HEADS, owners, block_span), 0, 1 << 20) * block_span + jnp.arange(block_span, dtype=jnp.int32)
    order = jnp.argsort(within, axis=-1)[:, :, :CAP]
    blocks = (order + jnp.arange(owners, dtype=jnp.int32)[None, :, None] * block_span).reshape(KEY_VALUE_HEADS, owners * CAP)
    owner_of = jnp.repeat(jnp.arange(owners, dtype=jnp.int32), CAP)
    forced_blocks = jax.random.randint(force_seed, (KEY_VALUE_HEADS, 1), 0, owners)
    block_score = jax.random.randint(score_seed, (KEY_VALUE_HEADS, owners * CAP), 0, 4096) + (owners - owner_of)[None, :] * (8192 // owners)
    block_score = block_score + jnp.where(owner_of[None, :] == forced_blocks, 1 << 16, 0)
    block_score = block_score * (owners * CAP) + jnp.arange(owners * CAP, dtype=jnp.int32)[None, :]
    unused, picked = lax.top_k(block_score, NV)
    chosen = jnp.take_along_axis(blocks, picked, axis=1)
    return jnp.sort(chosen, axis=1).astype(jnp.int32)


def draw_slash(key, part):
    block_span = S_DEV // BLK
    score_seed, force_seed = jax.random.split(jax.random.fold_in(key, 5), 2)
    block_score = jax.random.randint(score_seed, (KEY_VALUE_HEADS, block_span), 0, 4096) * block_span + jnp.arange(block_span, dtype=jnp.int32)[None, :]
    forced_blocks = jax.random.randint(force_seed, (), 0, KEY_VALUE_HEADS)
    extra_score = (jnp.arange(KEY_VALUE_HEADS)[:, None] == forced_blocks) & (jnp.arange(block_span)[None, :] == block_span - 1)
    block_score = block_score + jnp.where(extra_score, 1 << 24, 0)
    unused, picked = lax.top_k(block_score, NS)
    return jnp.sort(picked + 1, axis=1).astype(jnp.int32)


def block_scale(key, shape, pieces, least, top_value):
    def one(position, blocks):
        steps = jax.random.uniform(jax.random.fold_in(jax.random.fold_in(key, 6), position), (blocks,), jnp.float32, least / len(pieces), top_value / len(pieces))
        return jnp.repeat(jnp.exp(steps), shape[position] // blocks).reshape((-1,) + (1,) * (len(shape) - position - 1))

    loudness = one(*pieces[0])
    for cut in pieces[1:]:
        loudness = loudness * one(*cut)
    return loudness


def bell_draw(key, shape, scale, bound, pieces=(), held_as=jnp.bfloat16):
    factor_of = block_scale(key, shape, pieces, -0.22, 0.18) if pieces else 1.0
    array = jax.random.normal(key, shape, jnp.float32) * scale * factor_of
    return jnp.minimum(jnp.maximum(array, -bound), bound).astype(held_as)


def setup_inputs(seed: int = 0) -> dict:
    splits = jax.random.split(jax.random.key(seed), 7)
    return {
        "queries": draw_queries(jax.random.fold_in(splits[6], 71), 0),
        "keys": draw_keys(jax.random.fold_in(splits[6], 71), 0),
        "values": bell_draw(splits[2], (SEQ, KEY_VALUE_HEADS * HEAD_DIM), 1.0, 6.0, ((0, 16), (1, 2))),
        "vertical": draw_vertical(jax.random.fold_in(splits[6], 71), 0),
        "slash": draw_slash(jax.random.fold_in(splits[6], 71), 0),
        "out_weight": bell_draw(splits[5], (HEADS * HEAD_DIM, DMODEL), HEADS ** -0.5, 1.0, ((0, 2),)),
    }


NEGATIVE = -1e30


def attended_block_tile(block_index, vert_ids, slash_ids, key_head, value_head, query_head_index, causal):
    offsets = jnp.concatenate([jnp.zeros((1,), jnp.int32), slash_ids.astype(jnp.int32)])
    diagonal = block_index - offsets
    vert_ok = (vert_ids < block_index) & jnp.all(block_index - vert_ids[:, None] != slash_ids[None, :], axis=1)
    diag_ok = diagonal >= 0
    chosen = jnp.concatenate([vert_ids.astype(jnp.int32), jnp.maximum(diagonal, 0).astype(jnp.int32)])
    usable = jnp.concatenate([vert_ok, diag_ok])
    gathered_keys = key_head[chosen].reshape(-1, HEAD_DIM)
    gathered_values = value_head[chosen].reshape(-1, HEAD_DIM)
    same_block = chosen == block_index
    allowed = usable[None, :, None] & (jnp.logical_not(same_block)[None, :, None] | causal[:, None, :])
    allowed = allowed.reshape(BLK, -1)
    query_block_tile = query_head_index[block_index]
    scores = jnp.einsum("qgd,kd->gqk", query_block_tile.astype(jnp.float32), gathered_keys.astype(jnp.float32)) * (HEAD_DIM ** -0.5)
    scores = jnp.where(allowed[None], scores, NEGATIVE)
    top_score = jnp.max(scores, axis=-1, keepdims=True)
    weights = jnp.where(allowed[None], jnp.exp(scores - top_score), 0.0)
    sum_weight = jnp.sum(weights, axis=-1, keepdims=True)
    rounded = lax.optimization_barrier(weights.astype(jnp.bfloat16)).astype(jnp.float32)
    output = jnp.einsum("gqk,kd->gqd", rounded, gathered_values.astype(jnp.float32)) / sum_weight
    return output.transpose(1, 0, 2).astype(jnp.bfloat16)


def attend_slab(slab_start, block_fn, slab_blocks):
    return jax.vmap(block_fn)(slab_start + jnp.arange(slab_blocks, dtype=jnp.int32))


def reference(queries, keys, values, vertical, slash, out_weight):
    per_group = HEADS // KEY_VALUE_HEADS
    block_count = SEQ // BLK
    slab_blocks = S_DEV // BLK
    query_blocks = queries.reshape(block_count, BLK, KEY_VALUE_HEADS, per_group, HEAD_DIM)
    key_blocks = keys.reshape(block_count, BLK, KEY_VALUE_HEADS, HEAD_DIM)
    value_blocks = values.reshape(block_count, BLK, KEY_VALUE_HEADS, HEAD_DIM)
    within = jnp.arange(BLK)
    causal = within[None, :] <= within[:, None]
    results = []
    for head_index in range(KEY_VALUE_HEADS):
        block_fn = partial(attended_block_tile, vert_ids=vertical[head_index], slash_ids=slash[head_index],
                           key_head=key_blocks[:, :, head_index], value_head=value_blocks[:, :, head_index],
                           query_head_index=query_blocks[:, :, head_index], causal=causal)
        mapped = lax.map(partial(attend_slab, block_fn=block_fn, slab_blocks=slab_blocks),
                         jnp.arange(N_SEQ, dtype=jnp.int32) * slab_blocks)
        results.append(mapped.reshape(SEQ, per_group * HEAD_DIM))
    attention = jnp.concatenate(results, axis=1)
    return jnp.dot(attention, out_weight, preferred_element_type=jnp.float32).astype(jnp.bfloat16)
```

```python
import functools
import math

import jax
import jax.numpy as jnp
from jax import lax
from jax.experimental import pallas as pl
from jax.experimental.pallas import tpu as pltpu
from jax.sharding import PartitionSpec as P

HEAD_DIM = 128
BLK = 64
CAP = 2
NEGATIVE = -1e30
MESH = pl.DeviceIdType.MESH
SCALE = HEAD_DIM ** (-0.5) * math.log2(math.e)


def kernel(
    n, inner, kv, per_group, tile,
    q_ref, k_ref, v_ref, pack_ref, bias_ref, w_hbm, out_ref,
    slots, prev, w_ref, acc, top, total, attn, res, give, take,
    w_sem, prev_send, prev_recv, slot_recv, k_out, k_in, k_fwd, v_in, v_out, x_send, x_recv,
):
    rows = q_ref.shape[0]
    outer = n // inner
    me = lax.axis_index("seq")
    core = lax.axis_index("head")
    o, c = me // inner, me % inner
    other = 1 - core
    slab_blocks = rows // BLK
    half = rows // 2
    slot_keys = CAP * BLK

    barrier = pltpu.get_barrier_semaphore()

    def greet(seq, head):
        pl.semaphore_signal(barrier, inc=1, device_id=(seq, head), device_id_type=MESH)

    greet(me, other)
    for d in range(1, inner):
        greet(o * inner + (c + d) % inner, core)
    for d in range(1, outer):
        greet(((o + d) % outer) * inner + c, core)

    @pl.when(me + 1 < n)
    def _():
        greet(me + 1, core)

    @pl.when(me > 0)
    def _():
        greet(me - 1, core)

    weight_copy = pltpu.make_async_copy(w_hbm, w_ref, w_sem)
    weight_copy.start()
    pl.semaphore_wait(
        barrier,
        1 + (inner - 1) + (outer - 1) + jnp.where(me > 0, 1, 0) + jnp.where(me + 1 < n, 1, 0),
    )

    sends = []

    def remote(src, dst, send_sem, recv_sem, seq):
        return pltpu.make_async_remote_copy(
            src_ref=src, dst_ref=dst, send_sem=send_sem, recv_sem=recv_sem,
            device_id=(seq, core), device_id_type=MESH,
        )

    def launch(cond, *args):
        def begin():
            remote(*args).start()

        pl.when(cond)(begin)
        sends.append((cond, args))

    def arrived(slab, part):
        remote(slots.at[slab, part], slots.at[slab, part], k_out.at[0],
               slot_recv.at[slab, part], (me + 1) % n).wait_recv()

    for d in range(1, outer):
        launch(o + d < outer, pack_ref.at[0], slots.at[me, 0], k_out.at[d], slot_recv.at[me, 0],
               me + d * inner)
    for d in range(1, inner):
        peer = (c + d) % inner
        launch((o < outer - 1) | (peer > c), pack_ref.at[1], slots.at[me, 1], v_in.at[d],
               slot_recv.at[me, 1], o * inner + peer)
    for d in range(1, inner):
        peer = (c + d) % inner
        launch(peer > c, pack_ref.at[0], slots.at[me, 0], k_in.at[d], slot_recv.at[me, 0],
               o * inner + peer)
    for d in range(1, outer):
        launch(o + d < outer, pack_ref.at[1], slots.at[me, 1], v_out.at[0, d], slot_recv.at[me, 1],
               me + d * inner)
    launch(me + 1 < n, k_ref, prev.at[0], prev_send.at[0], prev_recv.at[0], me + 1)
    launch(me + 1 < n, v_ref, prev.at[1], prev_send.at[1], prev_recv.at[1], me + 1)

    def attend(get_k, get_v, bias_row, causal):
        def one_head(h, _):
            k = get_k(h)
            vt = get_v(h).T
            pieces = k.shape[0] // BLK
            for g in range(per_group):
                j = h * per_group + g
                q = q_ref[:, pl.ds(pl.multiple_of(j * HEAD_DIM, HEAD_DIM), HEAD_DIM)]
                s = lax.dot_general(k, q, (((1,), (1,)), ((), ())),
                                    preferred_element_type=jnp.float32) * SCALE
                parts = [
                    s[i * BLK:(i + 1) * BLK] + bias_ref[h, pl.ds(bias_row + i, 1), :]
                    for i in range(pieces)
                ]
                s = jnp.concatenate(parts, axis=0)
                if causal:
                    keys_at = lax.broadcasted_iota(jnp.int32, s.shape, 0)
                    query_at = lax.broadcasted_iota(jnp.int32, s.shape, 1)
                    s = jnp.where(keys_at <= query_at, s, NEGATIVE)
                peak = jnp.max(s, axis=0, keepdims=True)
                if causal:
                    p = jnp.exp2(s - peak)
                    top[j] = peak
                    total[j] = jnp.sum(p, axis=0, keepdims=True)
                    acc[j] = jnp.dot(vt, p.astype(jnp.bfloat16), preferred_element_type=jnp.float32)
                else:
                    before = top[j]
                    peak = jnp.maximum(before, peak)
                    shrink = jnp.exp2(before - peak)
                    p = jnp.exp2(s - peak)
                    top[j] = peak
                    total[j] = total[j] * shrink + jnp.sum(p, axis=0, keepdims=True)
                    acc[j] = acc[j] * shrink + jnp.dot(
                        vt, p.astype(jnp.bfloat16), preferred_element_type=jnp.float32)
            return 0

        lax.fori_loop(0, kv, one_head, 0)

    def lanes(h):
        return pl.ds(pl.multiple_of(h * HEAD_DIM, HEAD_DIM), HEAD_DIM)

    def attend_slots(slab, count):
        def get(part):
            return lambda h: jnp.concatenate(
                [slots[slab + i, part, :, lanes(h)] for i in range(count)], axis=0)

        attend(get(0), get(1), 2 * slab_blocks + slab * CAP, False)

    attend(lambda h: k_ref[:, lanes(h)], lambda h: v_ref[:, lanes(h)], 0, True)

    for d in range(1, max(inner, outer)):
        if d < outer:
            source = me - d * inner

            @pl.when(d <= o)
            def _(source=source):
                arrived(source, 0)

            for e in range(1, inner):
                launch(d <= o, slots.at[source, 0], slots.at[source, 0], k_fwd.at[d, e],
                       slot_recv.at[source, 0], o * inner + (c + e) % inner)
        if d < inner:
            peer = (c + inner - d) % inner
            source = o * inner + peer

            @pl.when((o < outer - 1) | (peer < c))
            def _(source=source):
                arrived(source, 1)

            for e in range(1, outer):
                launch(o + e < outer, slots.at[source, 1], slots.at[source, 1], v_out.at[d, e],
                       slot_recv.at[source, 1], me + e * inner)

    for near in range(inner - 1):
        @pl.when(near < c)
        def _(near=near):
            arrived(o * inner + near, 0)
            attend_slots(o * inner + near, 1)

    @pl.when(me > 0)
    def _():
        for i in range(2):
            remote(prev.at[i], prev.at[i], prev_send.at[i], prev_recv.at[i], (me + 1) % n).wait_recv()
        attend(lambda h: prev[0, :, lanes(h)], lambda h: prev[1, :, lanes(h)], slab_blocks, False)

    step = 2 if inner % 2 == 0 else 1

    def plane(d, _):
        base = (o - 1 - d) * inner
        for part in range(0, inner, step):
            for i in range(part, part + step):
                @pl.when(c != i)
                def _(i=i):
                    arrived(base + i, 0)

                arrived(base + i, 1)
            attend_slots(base + part, step)
        return 0

    lax.fori_loop(0, o, plane, 0)

    def finish(j, _):
        a = acc[j] / total[j]
        attn[:, lanes(j)] = a.T.astype(jnp.bfloat16)
        return 0

    lax.fori_loop(0, kv * per_group, finish, 0)
    weight_copy.wait()
    tiles = give.shape[0]
    mine = pl.ds(pl.multiple_of(core * half, half), half)
    theirs = pl.ds(pl.multiple_of(other * half, half), half)

    def swap(t):
        return pltpu.make_async_remote_copy(
            src_ref=give.at[t], dst_ref=take.at[t], send_sem=x_send.at[t], recv_sem=x_recv.at[t],
            device_id=(me, other), device_id_type=MESH,
        )

    def project(t, _):
        columns = pl.ds(pl.multiple_of(t * tile, tile), tile)
        res[t] = jnp.dot(attn[...], w_ref[:, columns], preferred_element_type=jnp.float32)
        give[t] = res[t, theirs, :].astype(jnp.bfloat16)
        swap(t).start()
        return 0

    lax.fori_loop(0, tiles, project, 0)

    def add_up(t, _):
        columns = pl.ds(pl.multiple_of(t * tile, tile), tile)
        swap(t).wait_recv()
        out_ref[:, columns] = (res[t, mine, :] + take[t].astype(jnp.float32)).astype(out_ref.dtype)
        return 0

    lax.fori_loop(0, tiles, add_up, 0)

    def sent(t, _):
        swap(t).wait_send()
        return 0

    lax.fori_loop(0, tiles, sent, 0)
    for cond, args in sends:
        def settle(args=args):
            remote(*args).wait_send()

        pl.when(cond)(settle)


def on_device(n, queries, keys, values, vertical, slash, out_weight):
    rows = queries.shape[0]
    kv = vertical.shape[0]
    per_group = queries.shape[1] // (kv * HEAD_DIM)
    slab_blocks = rows // BLK
    inner = math.gcd(n, 4)
    outer = n // inner
    model = out_weight.shape[1]
    my_slab = lax.axis_index("seq")
    first_block = my_slab * slab_blocks

    slab_ids = jnp.arange(n, dtype=jnp.int32)
    held_by = (vertical // slab_blocks)[:, None, :] == slab_ids[None, :, None]
    none = n * slab_blocks
    low = jnp.min(jnp.where(held_by, vertical[:, None, :], none), axis=-1)
    high = jnp.max(jnp.where(held_by, vertical[:, None, :], -1), axis=-1)
    slot_block = jnp.stack([low, jnp.where(high > low, high, none)], axis=-1).reshape(kv, n * CAP)
    local = jnp.arange(slab_blocks, dtype=jnp.int32)
    key_block = jnp.concatenate(
        [
            jnp.broadcast_to((first_block + local)[None], (kv, slab_blocks)),
            jnp.broadcast_to((first_block - slab_blocks + local)[None], (kv, slab_blocks)),
            slot_block,
        ],
        axis=1,
    )
    query_block = first_block + jnp.arange(rows, dtype=jnp.int32) // BLK
    gap = query_block[None, None, :] - key_block[:, :, None]
    on_slash = jnp.any(gap[..., None] == slash[:, None, None, :], axis=-1)
    row_ids = jnp.arange(key_block.shape[1])[None, :, None]
    chosen = jnp.any(key_block[:, :, None] == vertical[:, None, :], axis=-1)[:, :, None]
    later = gap > 0
    allowed = jnp.where(
        row_ids < slab_blocks,
        on_slash | (gap == 0) | (chosen & later),
        jnp.where(row_ids < 2 * slab_blocks, on_slash & (my_slab > 0), later & ~on_slash),
    )
    bias = jnp.where(allowed, 0.0, NEGATIVE).astype(jnp.float32)

    inside = (vertical // slab_blocks) == my_slab
    my_low = jnp.min(jnp.where(inside, vertical, none), axis=-1) - first_block
    my_high = jnp.max(jnp.where(inside, vertical, -1), axis=-1) - first_block
    pick = jnp.stack([my_low, my_high])
    pick = jnp.repeat(pick, HEAD_DIM, axis=1)[:, None, :]

    def packed(array):
        blocks = array.reshape(slab_blocks, BLK, kv * HEAD_DIM)
        chosen = jnp.broadcast_to(blocks[0][None], (CAP, BLK, kv * HEAD_DIM))
        for i in range(1, slab_blocks):
            chosen = jnp.where(pick == i, blocks[i][None], chosen)
        return chosen.reshape(CAP * BLK, kv * HEAD_DIM)

    pack = jnp.stack([packed(keys), packed(values)])

    tile = math.gcd(model, 512)
    tiles = model // tile
    heads = kv * per_group
    vmem = pl.BlockSpec(memory_space=pltpu.VMEM)
    dma = pltpu.SemaphoreType.DMA
    return pl.pallas_call(
        functools.partial(kernel, n, inner, kv, per_group, tile),
        out_shape=jax.ShapeDtypeStruct((rows // 2, model), jnp.bfloat16),
        in_specs=[vmem] * 5 + [pl.BlockSpec(memory_space=pl.ANY)],
        out_specs=vmem,
        scratch_shapes=[
            pltpu.VMEM((n, 2, CAP * BLK, kv * HEAD_DIM), jnp.bfloat16),
            pltpu.VMEM((2, rows, kv * HEAD_DIM), jnp.bfloat16),
            pltpu.VMEM(out_weight.shape, jnp.bfloat16),
            pltpu.VMEM((heads, HEAD_DIM, rows), jnp.float32),
            pltpu.VMEM((heads, 1, rows), jnp.float32),
            pltpu.VMEM((heads, 1, rows), jnp.float32),
            pltpu.VMEM((rows, heads * HEAD_DIM), jnp.bfloat16),
            pltpu.VMEM((tiles, rows, tile), jnp.float32),
            pltpu.VMEM((tiles, rows // 2, tile), jnp.bfloat16),
            pltpu.VMEM((tiles, rows // 2, tile), jnp.bfloat16),
            dma,
            dma((2,)),
            dma((2,)),
            dma((n, 2)),
            dma((outer,)),
            dma((inner,)),
            dma((outer, inner)),
            dma((inner,)),
            dma((inner, outer)),
            dma((tiles,)),
            dma((tiles,)),
        ],
        compiler_params=pltpu.CompilerParams(
            collective_id=0, has_side_effects=True, vmem_limit_bytes=60 * 2**20
        ),
    )(queries, keys, values, pack, bias, out_weight)


def solution(mesh):
    placed = (
        P("seq", "head"),
        P("seq", "head"),
        P("seq", "head"),
        P("head", None),
        P("head", None),
        P("head", None),
    )
    return jax.shard_map(
        functools.partial(on_device, mesh.shape["seq"]),
        mesh=mesh, in_specs=placed, out_specs=P(("seq", "head"), None), check_vma=False,
    )
```

```python
import functools
import math

import jax
import jax.numpy as jnp
from jax import lax
from jax.experimental import pallas as pl
from jax.experimental.pallas import tpu as pltpu
from jax.sharding import PartitionSpec as P

HEAD_DIM = 128
BLK = 64
CAP = 2
NEGATIVE = -1e30
MESH = pl.DeviceIdType.MESH
SCALE = HEAD_DIM ** (-0.5) * math.log2(math.e)


def kernel(
    n, inner, cut, kv, per_group, tile,
    q_ref, k_ref, v_ref, vert_ref, slash_ref, w_hbm, out_ref,
    pack_ref, bias_ref, slots, prev, w_ref, acc, top, total, attn, res, give, take,
    w_sem, prev_send, prev_recv, slot_recv, k_up, k_in, v_in, v_up, x_send, x_recv,
):
    rows = q_ref.shape[0]
    outer = n // inner
    me = lax.axis_index("seq")
    core = lax.axis_index("head")
    o, c = me // inner, me % inner
    other = 1 - core
    slab_blocks = rows // BLK
    half = rows // 2
    slot_keys = CAP * BLK

    barrier = pltpu.get_barrier_semaphore()

    def greet(seq, head):
        pl.semaphore_signal(barrier, inc=1, device_id=(seq, head), device_id_type=MESH)

    greet(me, other)
    for d in range(1, inner):
        greet(o * inner + (c + d) % inner, core)
    if outer > 1:
        greet((me + inner) % n, core)
        greet((me + n - inner) % n, core)

    @pl.when(me + 1 < n)
    def _():
        greet(me + 1, core)

    @pl.when(me > 0)
    def _():
        greet(me - 1, core)

    first_block = me * slab_blocks
    none = n * slab_blocks
    chosen_count = vert_ref.shape[1]
    for h in range(kv):
        low, high = jnp.int32(none), jnp.int32(-1)
        for i in range(chosen_count):
            block = vert_ref[h, i] - first_block
            inside = (block >= 0) & (block < slab_blocks)
            low = jnp.where(inside, jnp.minimum(low, block), low)
            high = jnp.where(inside, jnp.maximum(high, block), high)
        columns = slice(h * HEAD_DIM, (h + 1) * HEAD_DIM)
        for part, source in enumerate((k_ref, v_ref)):
            for slot, pick in enumerate((low, high)):
                got = source[:BLK, columns]
                for i in range(1, slab_blocks):
                    got = jnp.where(pick == i, source[i * BLK:(i + 1) * BLK, columns], got)
                at = part * slot_keys + slot * BLK
                pack_ref[at:at + BLK, columns] = got

    weight_copy = pltpu.make_async_copy(w_hbm, w_ref, w_sem)
    weight_copy.start()
    pl.semaphore_wait(
        barrier,
        1 + (inner - 1) + (2 if outer > 1 else 0) + jnp.where(me > 0, 1, 0) + jnp.where(me + 1 < n, 1, 0),
    )

    def remote(src, dst, send_sem, recv_sem, seq):
        return pltpu.make_async_remote_copy(
            src_ref=src, dst_ref=dst, send_sem=send_sem, recv_sem=recv_sem,
            device_id=(seq, core), device_id_type=MESH,
        )

    parts = (pl.ds(0, cut), pl.ds(cut, 2 * slot_keys - cut))
    above = (me + inner) % n

    def relay(slab, part, send_sem, seq, own=False):
        there = slots.at[slab, parts[part]]
        return remote(pack_ref.at[parts[part]] if own else there, there, send_sem,
                      slot_recv.at[slab, part], seq)

    def arrived(slab, part):
        relay(slab, part, k_up.at[0], above).wait_recv()

    def own_plane(act):
        for d in range(1, inner):
            peer = (c + d) % inner

            @pl.when((o < outer - 1) | (peer > c))
            def _(d=d, peer=peer):
                act(relay(me, 1, v_in.at[d], o * inner + peer, own=True))

        @pl.when(o < outer - 1)
        def _():
            act(relay(me, 0, k_up.at[0], above, own=True))

        for d in range(1, inner):
            peer = (c + d) % inner

            @pl.when(peer > c)
            def _(d=d, peer=peer):
                act(relay(me, 0, k_in.at[0, d], o * inner + peer, own=True))

        @pl.when(o < outer - 1)
        def _():
            act(relay(me, 1, v_up.at[0, 0], above, own=True))

        @pl.when(me + 1 < n)
        def _():
            for i, own in enumerate((k_ref, v_ref)):
                act(remote(own, prev.at[i], prev_send.at[i], prev_recv.at[i], me + 1))

    def spread_plane(d, start):
        act = (lambda copy: copy.start()) if start else (lambda copy: copy.wait_send())
        source = me - d * inner
        if start:
            arrived(source, 0)

        @pl.when(o < outer - 1)
        def _():
            act(relay(source, 0, k_up.at[d], above))

        for e in range(1, inner):
            act(relay(source, 0, k_in.at[d, e], o * inner + (c + e) % inner))
        for e in range(inner):
            slab = (o - d) * inner + (c + inner - e) % inner
            if start:
                arrived(slab, 1)

            @pl.when(o < outer - 1)
            def _(slab=slab, e=e):
                act(relay(slab, 1, v_up.at[d, e], above))

    own_plane(lambda copy: copy.start())

    def mask_rows(h, _):
        def filled(shape, value):
            return jnp.full(shape, value, jnp.int32)

        def on_slash(gap):
            hit = gap == slash_ref[h, 0]
            for i in range(1, slash_ref.shape[1]):
                hit = hit | (gap == slash_ref[h, i])
            return hit

        shape = (2 * slab_blocks, rows)
        row = lax.broadcasted_iota(jnp.int32, shape, 0)
        query_block = first_block + lax.broadcasted_iota(jnp.int32, shape, 1) // BLK
        block = first_block + jnp.where(row < slab_blocks, row, row - 2 * slab_blocks)
        gap = query_block - block

        def look(i, chosen):
            return jnp.where(block == vert_ref[h, i], 1, chosen)

        chosen = lax.fori_loop(0, chosen_count, look, filled(shape, 0))
        near = (gap == 0) | ((chosen > 0) & (gap > 0) & (row < slab_blocks))
        bias_ref[h, :2 * slab_blocks] = jnp.where(near | on_slash(gap), 0.0, NEGATIVE)

        shape = (n * CAP, rows)
        row = lax.broadcasted_iota(jnp.int32, shape, 0)
        query_block = first_block + lax.broadcasted_iota(jnp.int32, shape, 1) // BLK

        def extremes(i, found):
            low, high = found
            block = vert_ref[h, i]
            held = row // CAP == block // slab_blocks
            return (jnp.where(held, jnp.minimum(low, block), low),
                    jnp.where(held, jnp.maximum(high, block), high))

        low, high = lax.fori_loop(0, chosen_count, extremes, (filled(shape, none), filled(shape, -1)))
        block = jnp.where(row % CAP == 0, low, jnp.where(high > low, high, none))
        gap = query_block - block
        usable = jnp.where(on_slash(gap), 0, jnp.where(gap > 0, 1, 0))
        bias_ref[h, 2 * slab_blocks:] = jnp.where(usable > 0, 0.0, NEGATIVE)
        return 0

    lax.fori_loop(0, kv, mask_rows, 0)

    def attend(get_k, get_v, bias_row, causal):
        def one_head(h, _):
            k = get_k(h)
            vt = get_v(h).T
            pieces = k.shape[0] // BLK
            heads = [h * per_group + g for g in range(per_group)]
            rows_bias = [bias_ref[h, pl.ds(bias_row + i, 1), :] for i in range(pieces)]
            before = [None if causal else (top[j], total[j]) for j in heads]
            scores = []
            for j in heads:
                q = q_ref[:, pl.ds(pl.multiple_of(j * HEAD_DIM, HEAD_DIM), HEAD_DIM)]
                scores.append(lax.dot_general(k, q, (((1,), (1,)), ((), ())),
                                              preferred_element_type=jnp.float32))
            done = []
            for s, old in zip(scores, before):
                s = s * SCALE
                s = jnp.concatenate(
                    [s[i * BLK:(i + 1) * BLK] + rows_bias[i] for i in range(pieces)], axis=0)
                if causal:
                    keys_at = lax.broadcasted_iota(jnp.int32, s.shape, 0)
                    query_at = lax.broadcasted_iota(jnp.int32, s.shape, 1)
                    s = jnp.where(keys_at <= query_at, s, NEGATIVE)
                peak = jnp.max(s, axis=0, keepdims=True)
                shrink = None
                if not causal:
                    peak = jnp.maximum(old[0], peak)
                    shrink = jnp.exp2(old[0] - peak)
                p = jnp.exp2(s - peak)
                amount = jnp.sum(p, axis=0, keepdims=True)
                if not causal:
                    amount = old[1] * shrink + amount
                mix = jnp.dot(vt, p.astype(jnp.bfloat16), preferred_element_type=jnp.float32)
                done.append((peak, amount, shrink, mix))
            for j, (peak, amount, shrink, mix) in zip(heads, done):
                top[j] = peak
                total[j] = amount
                acc[j] = mix if causal else acc[j] * shrink + mix
            return 0

        lax.fori_loop(0, kv, one_head, 0)

    def lanes(h):
        return pl.ds(pl.multiple_of(h * HEAD_DIM, HEAD_DIM), HEAD_DIM)

    def attend_slots(slab, count):
        def get(first):
            return lambda h: jnp.concatenate(
                [slots[slab + i, first:first + slot_keys, lanes(h)] for i in range(count)], axis=0)

        attend(get(0), get(slot_keys), 2 * slab_blocks + slab * CAP, False)

    attend(lambda h: k_ref[:, lanes(h)], lambda h: v_ref[:, lanes(h)], 0, True)

    for e in range(1, inner):
        peer = (c + inner - e) % inner
        slab = o * inner + peer

        @pl.when((o < outer - 1) | (peer < c))
        def _(slab=slab):
            arrived(slab, 1)

        @pl.when(o < outer - 1)
        def _(slab=slab, e=e):
            relay(slab, 1, v_up.at[0, e], above).start()

    @pl.when(o > 0)
    def _():
        spread_plane(1, True)

    for near in range(inner - 1):
        @pl.when(near < c)
        def _(near=near):
            arrived(o * inner + near, 0)
            attend_slots(o * inner + near, 1)

    @pl.when(me > 0)
    def _():
        for i in range(2):
            remote(prev.at[i], prev.at[i], prev_send.at[i], prev_recv.at[i], above).wait_recv()
        attend(lambda h: prev[0, :, lanes(h)], lambda h: prev[1, :, lanes(h)], slab_blocks, False)

    step = 2 if inner % 2 == 0 else 1

    def plane(d, _):
        @pl.when(d < o)
        def _():
            spread_plane(d + 1, True)

        base = (o - d) * inner
        for part in range(0, inner, step):
            for i in range(part, part + step):
                @pl.when(c != i)
                def _(i=i):
                    arrived(base + i, 0)

            attend_slots(base + part, step)
        return 0

    lax.fori_loop(1, o + 1, plane, 0)

    def finish(j, _):
        a = acc[j] / total[j]
        attn[:, lanes(j)] = a.T.astype(jnp.bfloat16)
        return 0

    lax.fori_loop(0, kv * per_group, finish, 0)
    weight_copy.wait()
    tiles = give.shape[0]
    mine = pl.ds(pl.multiple_of(core * half, half), half)
    theirs = pl.ds(pl.multiple_of(other * half, half), half)

    def swap(t):
        return pltpu.make_async_remote_copy(
            src_ref=give.at[t], dst_ref=take.at[t], send_sem=x_send.at[t], recv_sem=x_recv.at[t],
            device_id=(me, other), device_id_type=MESH,
        )

    def project(t, _):
        columns = pl.ds(pl.multiple_of(t * tile, tile), tile)
        res[t] = jnp.dot(attn[...], w_ref[:, columns], preferred_element_type=jnp.float32)
        give[t] = res[t, theirs, :].astype(jnp.bfloat16)
        swap(t).start()
        return 0

    lax.fori_loop(0, tiles, project, 0)

    def add_up(t, _):
        columns = pl.ds(pl.multiple_of(t * tile, tile), tile)
        swap(t).wait_recv()
        out_ref[:, columns] = (res[t, mine, :] + take[t].astype(jnp.float32)).astype(out_ref.dtype)
        return 0

    lax.fori_loop(0, tiles, add_up, 0)

    def sent(t, _):
        swap(t).wait_send()
        return 0

    lax.fori_loop(0, tiles, sent, 0)
    own_plane(lambda copy: copy.wait_send())
    for e in range(1, inner):
        @pl.when(o < outer - 1)
        def _(e=e):
            relay(o * inner + (c + inner - e) % inner, 1, v_up.at[0, e], above).wait_send()

    def left(d, _):
        spread_plane(d, False)
        return 0

    lax.fori_loop(1, o + 1, left, 0)


def on_device(n, queries, keys, values, vertical, slash, out_weight):
    rows = queries.shape[0]
    kv = vertical.shape[0]
    per_group = queries.shape[1] // (kv * HEAD_DIM)
    slab_blocks = rows // BLK
    inner = math.gcd(n, 4)
    outer = n // inner
    model = out_weight.shape[1]
    cut = CAP * BLK + CAP * BLK // 2

    tile = math.gcd(model, 512)
    tiles = model // tile
    heads = kv * per_group
    vmem = pl.BlockSpec(memory_space=pltpu.VMEM)
    smem = pl.BlockSpec(memory_space=pltpu.SMEM)
    dma = pltpu.SemaphoreType.DMA
    return pl.pallas_call(
        functools.partial(kernel, n, inner, cut, kv, per_group, tile),
        out_shape=jax.ShapeDtypeStruct((rows // 2, model), jnp.bfloat16),
        in_specs=[vmem] * 3 + [smem] * 2 + [pl.BlockSpec(memory_space=pl.ANY)],
        out_specs=vmem,
        scratch_shapes=[
            pltpu.VMEM((2 * CAP * BLK, kv * HEAD_DIM), jnp.bfloat16),
            pltpu.VMEM((kv, 2 * slab_blocks + n * CAP, rows), jnp.float32),
            pltpu.VMEM((n, 2 * CAP * BLK, kv * HEAD_DIM), jnp.bfloat16),
            pltpu.VMEM((2, rows, kv * HEAD_DIM), jnp.bfloat16),
            pltpu.VMEM(out_weight.shape, jnp.bfloat16),
            pltpu.VMEM((heads, HEAD_DIM, rows), jnp.float32),
            pltpu.VMEM((heads, 1, rows), jnp.float32),
            pltpu.VMEM((heads, 1, rows), jnp.float32),
            pltpu.VMEM((rows, heads * HEAD_DIM), jnp.bfloat16),
            pltpu.VMEM((tiles, rows, tile), jnp.float32),
            pltpu.VMEM((tiles, rows // 2, tile), jnp.bfloat16),
            pltpu.VMEM((tiles, rows // 2, tile), jnp.bfloat16),
            dma,
            dma((2,)),
            dma((2,)),
            dma((n, 2)),
            dma((outer,)),
            dma((outer, inner)),
            dma((inner,)),
            dma((outer, inner)),
            dma((tiles,)),
            dma((tiles,)),
        ],
        compiler_params=pltpu.CompilerParams(
            collective_id=0, has_side_effects=True, vmem_limit_bytes=60 * 2**20
        ),
    )(queries, keys, values, vertical, slash, out_weight)


def solution(mesh):
    placed = (
        P("seq", "head"),
        P("seq", "head"),
        P("seq", "head"),
        P("head", None),
        P("head", None),
        P("head", None),
    )
    return jax.shard_map(
        functools.partial(on_device, mesh.shape["seq"]),
        mesh=mesh, in_specs=placed, out_specs=P(("seq", "head"), None), check_vma=False,
    )
```

```python
import functools
import math

import jax
import jax.numpy as jnp
from jax import lax
from jax.experimental import pallas as pl
from jax.experimental.pallas import tpu as pltpu
from jax.sharding import PartitionSpec as P

HEAD_DIM = 128
BLK = 64
CAP = 2
NEGATIVE = -1e30
MESH = pl.DeviceIdType.MESH
SCALE = HEAD_DIM ** (-0.5) * math.log2(math.e)


def kernel(
    n, inner, cut, kv, per_group, tile,
    q_ref, k_ref, v_ref, vert_ref, slash_ref, w_hbm, out_ref,
    pack_ref, bias_ref, slots, prev, w_ref, acc, top, total, attn, res, give, take,
    w_sem, prev_send, prev_recv, slot_recv, k_up, k_in, v_in, v_up, x_send, x_recv,
):
    rows = q_ref.shape[0]
    outer = n // inner
    me = lax.axis_index("seq")
    core = lax.axis_index("head")
    o, c = me // inner, me % inner
    other = 1 - core
    slab_blocks = rows // BLK
    half = rows // 2
    slot_keys = CAP * BLK

    barrier = pltpu.get_barrier_semaphore()

    def greet(seq, head):
        pl.semaphore_signal(barrier, inc=1, device_id=(seq, head), device_id_type=MESH)

    greet(me, other)
    for d in range(1, inner):
        greet(o * inner + (c + d) % inner, core)
    if outer > 1:
        greet((me + inner) % n, core)
        greet((me + n - inner) % n, core)

    @pl.when(me + 1 < n)
    def _():
        greet(me + 1, core)

    @pl.when(me > 0)
    def _():
        greet(me - 1, core)

    first_block = me * slab_blocks
    none = n * slab_blocks
    chosen_count = vert_ref.shape[1]
    for h in range(kv):
        low, high = jnp.int32(none), jnp.int32(-1)
        for i in range(chosen_count):
            block = vert_ref[h, i] - first_block
            inside = (block >= 0) & (block < slab_blocks)
            low = jnp.where(inside, jnp.minimum(low, block), low)
            high = jnp.where(inside, jnp.maximum(high, block), high)
        columns = slice(h * HEAD_DIM, (h + 1) * HEAD_DIM)
        for part, source in enumerate((k_ref, v_ref)):
            for slot, pick in enumerate((low, high)):
                got = source[:BLK, columns]
                for i in range(1, slab_blocks):
                    got = jnp.where(pick == i, source[i * BLK:(i + 1) * BLK, columns], got)
                at = part * slot_keys + slot * BLK
                pack_ref[at:at + BLK, columns] = got

    weight_copy = pltpu.make_async_copy(w_hbm, w_ref, w_sem)
    weight_copy.start()
    pl.semaphore_wait(
        barrier,
        1 + (inner - 1) + (2 if outer > 1 else 0) + jnp.where(me > 0, 1, 0) + jnp.where(me + 1 < n, 1, 0),
    )

    def remote(src, dst, send_sem, recv_sem, seq):
        return pltpu.make_async_remote_copy(
            src_ref=src, dst_ref=dst, send_sem=send_sem, recv_sem=recv_sem,
            device_id=(seq, core), device_id_type=MESH,
        )

    parts = (pl.ds(0, cut), pl.ds(cut, 2 * slot_keys - cut))
    above = (me + inner) % n

    def relay(slab, part, send_sem, seq, own=False):
        there = slots.at[slab, parts[part]]
        return remote(pack_ref.at[parts[part]] if own else there, there, send_sem,
                      slot_recv.at[slab, part], seq)

    def arrived(slab, part):
        relay(slab, part, k_up.at[0], above).wait_recv()

    def own_plane(act):
        for d in range(1, inner):
            peer = (c + d) % inner

            @pl.when((o < outer - 1) | (peer > c))
            def _(d=d, peer=peer):
                act(relay(me, 1, v_in.at[d], o * inner + peer, own=True))

        @pl.when(o < outer - 1)
        def _():
            act(relay(me, 0, k_up.at[0], above, own=True))

        for d in range(1, inner):
            peer = (c + d) % inner

            @pl.when(peer > c)
            def _(d=d, peer=peer):
                act(relay(me, 0, k_in.at[0, d], o * inner + peer, own=True))

        @pl.when(o < outer - 1)
        def _():
            act(relay(me, 1, v_up.at[0, 0], above, own=True))

        @pl.when(me + 1 < n)
        def _():
            for i, own in enumerate((k_ref, v_ref)):
                act(remote(own, prev.at[i], prev_send.at[i], prev_recv.at[i], me + 1))

    def spread_plane(d, start):
        act = (lambda copy: copy.start()) if start else (lambda copy: copy.wait_send())
        source = me - d * inner
        if start:
            arrived(source, 0)

        @pl.when(o < outer - 1)
        def _():
            act(relay(source, 0, k_up.at[d], above))

        for e in range(1, inner):
            act(relay(source, 0, k_in.at[d, e], o * inner + (c + e) % inner))
        for e in range(inner):
            slab = (o - d) * inner + (c + inner - e) % inner
            if start:
                arrived(slab, 1)

            @pl.when(o < outer - 1)
            def _(slab=slab, e=e):
                act(relay(slab, 1, v_up.at[d, e], above))

    own_plane(lambda copy: copy.start())

    def mask_rows(h, _):
        def filled(shape, value):
            return jnp.full(shape, value, jnp.int32)

        def on_slash(gap):
            hit = gap == slash_ref[h, 0]
            for i in range(1, slash_ref.shape[1]):
                hit = hit | (gap == slash_ref[h, i])
            return hit

        shape = (2 * slab_blocks, rows)
        row = lax.broadcasted_iota(jnp.int32, shape, 0)
        query_block = first_block + lax.broadcasted_iota(jnp.int32, shape, 1) // BLK
        block = first_block + jnp.where(row < slab_blocks, row, row - 2 * slab_blocks)
        gap = query_block - block

        def look(i, chosen):
            return jnp.where(block == vert_ref[h, i], 1, chosen)

        chosen = lax.fori_loop(0, chosen_count, look, filled(shape, 0))
        near = (gap == 0) | ((chosen > 0) & (gap > 0) & (row < slab_blocks))
        bias_ref[h, :2 * slab_blocks] = jnp.where(near | on_slash(gap), 0.0, NEGATIVE)

        shape = (n * CAP, rows)
        row = lax.broadcasted_iota(jnp.int32, shape, 0)
        query_block = first_block + lax.broadcasted_iota(jnp.int32, shape, 1) // BLK

        def extremes(i, found):
            low, high = found
            block = vert_ref[h, i]
            held = row // CAP == block // slab_blocks
            return (jnp.where(held, jnp.minimum(low, block), low),
                    jnp.where(held, jnp.maximum(high, block), high))

        low, high = lax.fori_loop(0, chosen_count, extremes, (filled(shape, none), filled(shape, -1)))
        block = jnp.where(row % CAP == 0, low, jnp.where(high > low, high, none))
        gap = query_block - block
        usable = jnp.where(on_slash(gap), 0, jnp.where(gap > 0, 1, 0))
        bias_ref[h, 2 * slab_blocks:] = jnp.where(usable > 0, 0.0, NEGATIVE)
        return 0

    lax.fori_loop(0, kv, mask_rows, 0)

    def attend(get_k, get_v, bias_row, causal):
        def one_head(h, _):
            k = get_k(h)
            vt = get_v(h).T
            pieces = k.shape[0] // BLK
            heads = [h * per_group + g for g in range(per_group)]
            rows_bias = [bias_ref[h, pl.ds(bias_row + i, 1), :] for i in range(pieces)]
            before = [None if causal else (top[j], total[j]) for j in heads]
            scores = []
            for j in heads:
                q = q_ref[:, pl.ds(pl.multiple_of(j * HEAD_DIM, HEAD_DIM), HEAD_DIM)]
                scores.append(lax.dot_general(k, q, (((1,), (1,)), ((), ())),
                                              preferred_element_type=jnp.float32))
            done = []
            for s, old in zip(scores, before):
                s = s * SCALE
                s = jnp.concatenate(
                    [s[i * BLK:(i + 1) * BLK] + rows_bias[i] for i in range(pieces)], axis=0)
                if causal:
                    keys_at = lax.broadcasted_iota(jnp.int32, s.shape, 0)
                    query_at = lax.broadcasted_iota(jnp.int32, s.shape, 1)
                    s = jnp.where(keys_at <= query_at, s, NEGATIVE)
                peak = jnp.max(s, axis=0, keepdims=True)
                shrink = None
                if not causal:
                    peak = jnp.maximum(old[0], peak)
                    shrink = jnp.exp2(old[0] - peak)
                p = jnp.exp2(s - peak)
                amount = jnp.sum(p, axis=0, keepdims=True)
                if not causal:
                    amount = old[1] * shrink + amount
                mix = jnp.dot(vt, p.astype(jnp.bfloat16), preferred_element_type=jnp.float32)
                done.append((peak, amount, shrink, mix))
            for j, (peak, amount, shrink, mix) in zip(heads, done):
                top[j] = peak
                total[j] = amount
                acc[j] = mix if causal else acc[j] * shrink + mix
            return 0

        lax.fori_loop(0, kv, one_head, 0)

    def lanes(h):
        return pl.ds(pl.multiple_of(h * HEAD_DIM, HEAD_DIM), HEAD_DIM)

    def attend_slots(slab, count):
        def get(first):
            return lambda h: jnp.concatenate(
                [slots[slab + i, first:first + slot_keys, lanes(h)] for i in range(count)], axis=0)

        attend(get(0), get(slot_keys), 2 * slab_blocks + slab * CAP, False)

    attend(lambda h: k_ref[:, lanes(h)], lambda h: v_ref[:, lanes(h)], 0, True)

    for e in range(1, inner):
        peer = (c + inner - e) % inner
        slab = o * inner + peer

        @pl.when((o < outer - 1) | (peer < c))
        def _(slab=slab):
            arrived(slab, 1)

        @pl.when(o < outer - 1)
        def _(slab=slab, e=e):
            relay(slab, 1, v_up.at[0, e], above).start()

    @pl.when(o > 0)
    def _():
        spread_plane(1, True)

    for near in range(inner - 1):
        @pl.when(near < c)
        def _(near=near):
            arrived(o * inner + near, 0)
            attend_slots(o * inner + near, 1)

    @pl.when(me > 0)
    def _():
        for i in range(2):
            remote(prev.at[i], prev.at[i], prev_send.at[i], prev_recv.at[i], above).wait_recv()
        attend(lambda h: prev[0, :, lanes(h)], lambda h: prev[1, :, lanes(h)], slab_blocks, False)

    step = inner

    def plane(d, _):
        @pl.when(d < o)
        def _():
            spread_plane(d + 1, True)

        base = (o - d) * inner
        for part in range(0, inner, step):
            for i in range(part, part + step):
                @pl.when(c != i)
                def _(i=i):
                    arrived(base + i, 0)

            attend_slots(base + part, step)
        return 0

    lax.fori_loop(1, o + 1, plane, 0)

    def finish(j, _):
        a = acc[j] / total[j]
        attn[:, lanes(j)] = a.T.astype(jnp.bfloat16)
        return 0

    lax.fori_loop(0, kv * per_group, finish, 0)
    weight_copy.wait()
    tiles = give.shape[0]
    mine = pl.ds(pl.multiple_of(core * half, half), half)
    theirs = pl.ds(pl.multiple_of(other * half, half), half)

    def swap(t):
        return pltpu.make_async_remote_copy(
            src_ref=give.at[t], dst_ref=take.at[t], send_sem=x_send.at[t], recv_sem=x_recv.at[t],
            device_id=(me, other), device_id_type=MESH,
        )

    def project(t, _):
        columns = pl.ds(pl.multiple_of(t * tile, tile), tile)
        res[t] = jnp.dot(attn[...], w_ref[:, columns], preferred_element_type=jnp.float32)
        give[t] = res[t, theirs, :].astype(jnp.bfloat16)
        swap(t).start()
        return 0

    lax.fori_loop(0, tiles, project, 0)

    def add_up(t, _):
        columns = pl.ds(pl.multiple_of(t * tile, tile), tile)
        swap(t).wait_recv()
        out_ref[:, columns] = (res[t, mine, :] + take[t].astype(jnp.float32)).astype(out_ref.dtype)
        return 0

    lax.fori_loop(0, tiles, add_up, 0)

    def sent(t, _):
        swap(t).wait_send()
        return 0

    lax.fori_loop(0, tiles, sent, 0)
    own_plane(lambda copy: copy.wait_send())
    for e in range(1, inner):
        @pl.when(o < outer - 1)
        def _(e=e):
            relay(o * inner + (c + inner - e) % inner, 1, v_up.at[0, e], above).wait_send()

    def left(d, _):
        spread_plane(d, False)
        return 0

    lax.fori_loop(1, o + 1, left, 0)


def on_device(n, queries, keys, values, vertical, slash, out_weight):
    rows = queries.shape[0]
    kv = vertical.shape[0]
    per_group = queries.shape[1] // (kv * HEAD_DIM)
    slab_blocks = rows // BLK
    inner = math.gcd(n, 4)
    outer = n // inner
    model = out_weight.shape[1]
    cut = CAP * BLK + CAP * BLK // 8 * 3

    tile = math.gcd(model, 512)
    tiles = model // tile
    heads = kv * per_group
    vmem = pl.BlockSpec(memory_space=pltpu.VMEM)
    smem = pl.BlockSpec(memory_space=pltpu.SMEM)
    dma = pltpu.SemaphoreType.DMA
    return pl.pallas_call(
        functools.partial(kernel, n, inner, cut, kv, per_group, tile),
        out_shape=jax.ShapeDtypeStruct((rows // 2, model), jnp.bfloat16),
        in_specs=[vmem] * 3 + [smem] * 2 + [pl.BlockSpec(memory_space=pl.ANY)],
        out_specs=vmem,
        scratch_shapes=[
            pltpu.VMEM((2 * CAP * BLK, kv * HEAD_DIM), jnp.bfloat16),
            pltpu.VMEM((kv, 2 * slab_blocks + n * CAP, rows), jnp.float32),
            pltpu.VMEM((n, 2 * CAP * BLK, kv * HEAD_DIM), jnp.bfloat16),
            pltpu.VMEM((2, rows, kv * HEAD_DIM), jnp.bfloat16),
            pltpu.VMEM(out_weight.shape, jnp.bfloat16),
            pltpu.VMEM((heads, HEAD_DIM, rows), jnp.float32),
            pltpu.VMEM((heads, 1, rows), jnp.float32),
            pltpu.VMEM((heads, 1, rows), jnp.float32),
            pltpu.VMEM((rows, heads * HEAD_DIM), jnp.bfloat16),
            pltpu.VMEM((tiles, rows, tile), jnp.float32),
            pltpu.VMEM((tiles, rows // 2, tile), jnp.bfloat16),
            pltpu.VMEM((tiles, rows // 2, tile), jnp.bfloat16),
            dma,
            dma((2,)),
            dma((2,)),
            dma((n, 2)),
            dma((outer,)),
            dma((outer, inner)),
            dma((inner,)),
            dma((outer, inner)),
            dma((tiles,)),
            dma((tiles,)),
        ],
        compiler_params=pltpu.CompilerParams(
            collective_id=0, has_side_effects=True, vmem_limit_bytes=60 * 2**20
        ),
    )(queries, keys, values, vertical, slash, out_weight)


def solution(mesh):
    placed = (
        P("seq", "head"),
        P("seq", "head"),
        P("seq", "head"),
        P("head", None),
        P("head", None),
        P("head", None),
    )
    return jax.shard_map(
        functools.partial(on_device, mesh.shape["seq"]),
        mesh=mesh, in_specs=placed, out_specs=P(("seq", "head"), None), check_vma=False,
    )
```
